32 devices in a mesh: gx: 4 (over y, x), gy: 2 (over core), gz: 4 (over z).
Axes of the slice: x: 2, y: 2, z: 4, core: 2. Of those that a mesh axis runs over, the one named last changes fastest.
Arguments:
- old_pos: float32 [3, 4, 2, 4, 1536], P(None, 'gx', 'gy', 'gz'), may hold values from -6 to 6
- displacement: float32 [3, 4, 2, 4, 1536], P(None, 'gx', 'gy', 'gz'), may hold values from -0.3 to 0.3
- inv_mass: float32 [4, 2, 4, 1536], P('gx', 'gy', 'gz'), may hold values from 0.0625 to 1
- bond_head: int32 [4, 2, 4, 1024], P('gx', 'gy', 'gz'), may hold values from 0 to 1535, as said below
- bond_tail: int32 [4, 2, 4, 1024], P('gx', 'gy', 'gz'), may hold values from 0 to 1967, as said below
- send_list: int32 [4, 2, 4, 16], P('gx', 'gy', 'gz'), may hold values from 0 to 1535, as said below
Outputs:
- new_pos: float32 [3, 4, 2, 4, 1536], P(None, 'gx', 'gy', 'gz')
- multipliers: float32 [4, 2, 4, 1024], P('gx', 'gy', 'gz')
The draws below stay inside these ranges and needn't reach their ends.
Inputs may be any that keep to these rules, and one draw needn't show every extreme that they name: `bond_head`: distinct atoms of the owning domain; no atom is the first atom of two constraints. `bond_tail`: below 1536: an atom of the owning domain other than the constraint's first atom, never in send_list; otherwise a slot 1536 + block * 16 + entry with block in 0..26 other than 13, distinct within a domain; 192 constraints of each domain use such slots. `send_list`: distinct atoms of the domain; a send atom is never a constraint's first atom and never a local second atom.
All inputs are finite; a program needn't handle non-finite values.
Results may differ from the reference program's by a relative error of at most 0.0011.
Values sent between devices are 32-bit elements; how exact they have to be, the bound alone decides.
A program may use at most 64 MiB of HBM per device.

```python
import math
import jax
import jax.numpy as jnp
from jax import lax

ATOM_DEV = 1536
CON_DEV = 1024
SEND = 16
HALO_CON = 192
ORDER = 4
DOM_X = 4
DOM_Y = 2
DOM_Z = 4


def layout(key):
    base = jax.random.fold_in(key, 7)
    keys = jax.random.split(base, DOM_X * DOM_Y * DOM_Z)

    def domain(dom_key):
        key_perm, key_pick, key_slot = jax.random.split(dom_key, 3)
        order = jax.random.permutation(key_perm, ATOM_DEV).astype(jnp.int32)
        sending = order[ATOM_DEV - SEND:]
        heads = order[:CON_DEV]
        local_tail = order[1:CON_DEV + 1]
        picked = jax.random.permutation(key_pick, CON_DEV).astype(jnp.int32)[:HALO_CON]
        slots = jax.random.permutation(key_slot, 26 * SEND).astype(jnp.int32)[:HALO_CON]
        block = slots // SEND
        block = block + (block >= 13).astype(jnp.int32)
        halo_tail = ATOM_DEV + block * SEND + slots % SEND
        tails = local_tail.at[picked].set(halo_tail.astype(jnp.int32))
        return (sending, heads, tails)
    sending, heads, tails = jax.vmap(domain)(keys)
    return (sending.reshape(DOM_X, DOM_Y, DOM_Z, SEND).astype(jnp.int32), heads.reshape(DOM_X, DOM_Y, DOM_Z, CON_DEV).astype(jnp.int32), tails.reshape(DOM_X, DOM_Y, DOM_Z, CON_DEV).astype(jnp.int32))


def draw_bond_head(key, part):
    return layout(key)[1]


def draw_bond_tail(key, part):
    return layout(key)[2]


def draw_send_list(key, part):
    return layout(key)[0]


def block_scale(own_key, shape, cuts, smallest, high):
    def one(position, shards_of):
        heights = jax.random.uniform(jax.random.fold_in(jax.random.fold_in(own_key, 6), position), (shards_of,), jnp.float32, smallest / len(cuts), high / len(cuts))
        return jnp.repeat(jnp.exp(heights), shape[position] // shards_of).reshape((-1,) + (1,) * (len(shape) - position - 1))

    factor_of = one(*cuts[0])
    for cut in cuts[1:]:
        factor_of = factor_of * one(*cut)
    return factor_of


def scatter_about(rng, extent, width, most, pieces=(), kind=jnp.bfloat16):
    array = jax.random.normal(rng, extent, jnp.float32) * width
    if len(pieces) > 0:
        array = block_scale(rng, extent, pieces, -0.22, 0.18) * array
    return jnp.clip(array, min=-most, max=most).astype(kind)


def setup_inputs(seed: int = 0) -> dict:
    splits = jax.random.split(jax.random.key(seed), 7)
    old_pos = scatter_about(splits[0], (3, DOM_X, DOM_Y, DOM_Z, ATOM_DEV), 1.0, 6.0, ((1, 4), (2, 2), (3, 4)), jnp.float32)
    displacement = scatter_about(splits[1], (3, DOM_X, DOM_Y, DOM_Z, ATOM_DEV), 0.05, 0.3, ((1, 4), (2, 2), (3, 4)), jnp.float32)
    inv_mass = jnp.clip(jnp.exp(math.log(1.0) - 2.7725887 * jax.random.uniform(splits[2], (DOM_X, DOM_Y, DOM_Z, ATOM_DEV), jnp.float32) ** block_scale(splits[2], (DOM_X, DOM_Y, DOM_Z, ATOM_DEV), ((0, 4), (1, 2), (2, 4)), -0.2, 0.2)), 0.0625, 1.0)
    bond_head = draw_bond_head(jax.random.fold_in(splits[6], 71), 0)
    bond_tail = draw_bond_tail(jax.random.fold_in(splits[6], 71), 0)
    send_list = draw_send_list(jax.random.fold_in(splits[6], 71), 0)
    return {"old_pos": old_pos, "displacement": displacement, "inv_mass": inv_mass, "bond_head": bond_head, "bond_tail": bond_tail, "send_list": send_list}


def global_index(bond_head, bond_tail, send_list):
    axis_x = jnp.arange(DOM_X, dtype=jnp.int32)[:, None, None, None]
    axis_y = jnp.arange(DOM_Y, dtype=jnp.int32)[None, :, None, None]
    axis_z = jnp.arange(DOM_Z, dtype=jnp.int32)[None, None, :, None]
    flat_dev = (axis_x * DOM_Y + axis_y) * DOM_Z + axis_z
    head = (flat_dev * ATOM_DEV + bond_head).reshape(-1)
    is_local = bond_tail < ATOM_DEV
    slot = jnp.maximum(bond_tail - ATOM_DEV, 0)
    block = slot // SEND
    entry = slot % SEND
    near_x = (axis_x + block // 9 - 1) % DOM_X
    near_y = (axis_y + block // 3 % 3 - 1) % DOM_Y
    near_z = (axis_z + block % 3 - 1) % DOM_Z
    neigh = (near_x * DOM_Y + near_y) * DOM_Z + near_z
    remote = send_list.reshape(-1)[(neigh * SEND + entry).reshape(-1)].reshape(neigh.shape)
    tail = jnp.where(is_local, flat_dev * ATOM_DEV + bond_tail, neigh * ATOM_DEV + remote)
    return (head.astype(jnp.int32), tail.reshape(-1).astype(jnp.int32))

def reference(old_pos, displacement, inv_mass, bond_head, bond_tail, send_list):
    head, tail = global_index(bond_head, bond_tail, send_list)
    old_flat = old_pos.reshape(3, -1)
    pos_now = old_flat + displacement.reshape(3, -1)
    masses = inv_mass.reshape(1, -1)
    total_atoms = old_flat.shape[1]
    bond_old = old_flat[:, head] - old_flat[:, tail]
    length = jnp.maximum(jnp.sqrt(lax.optimization_barrier(jnp.sum(bond_old * bond_old, axis=0))), 0.5)
    direction = bond_old / length
    bond_scale = 1.0 / jnp.sqrt(masses[0, head] + masses[0, tail])

    def spread(values):
        weighted = bond_scale * values * direction
        buffer = jnp.zeros((3, total_atoms), jnp.float32)
        buffer = buffer.at[:, head].add(weighted).at[:, tail].add(-weighted)
        return masses * buffer

    def couple(values):
        shift_vec = spread(values)
        return values - bond_scale * lax.optimization_barrier(jnp.sum(direction * (shift_vec[:, head] - shift_vec[:, tail]), axis=0))

    def expand(right_side):
        solution = right_side
        series = right_side
        for sweep in range(ORDER):
            series = couple(series)
            solution = solution + series
        return solution
    right_one = bond_scale * (lax.optimization_barrier(jnp.sum(direction * (pos_now[:, head] - pos_now[:, tail]), axis=0)) - length)
    sol_one = expand(right_one)
    pos_now = pos_now - spread(sol_one)
    stretch = pos_now[:, head] - pos_now[:, tail]
    current = lax.optimization_barrier(jnp.sum(stretch * stretch, axis=0))
    target = jnp.sqrt(jnp.maximum(2.0 * length * length - current, 0.5 * length * length))
    sol_two = expand(bond_scale * (length - target))
    pos_now = pos_now - spread(sol_two)
    return (pos_now.reshape(old_pos.shape), (sol_one + sol_two).reshape(bond_head.shape))
```

```python
import functools
import itertools

import jax
import jax.numpy as jnp
from jax import lax
from jax.experimental import pallas as pl
from jax.experimental.pallas import tpu as pltpu
from jax.sharding import PartitionSpec as P

ORDER = 4
LANES = 128
F32, BF16 = jnp.float32, jnp.bfloat16
MESH = pl.DeviceIdType.MESH


def pieces(value):
    high = value.astype(BF16).astype(F32)
    rest = value - high
    middle = rest.astype(BF16).astype(F32)
    return jnp.concatenate([high, middle, rest - middle], axis=0).astype(BF16)


def fold(out):
    rows = out.shape[0] // 3
    return out[:rows] + out[rows : 2 * rows] + out[2 * rows :]


def dot_nt(left, right):
    return lax.dot_general(left, right, (((1,), (1,)), ((), ())), preferred_element_type=F32)


def dot_nn(left, right):
    return lax.dot_general(left, right, (((1,), (0,)), ((), ())), preferred_element_type=F32)


def rows8(parts):
    count = sum(part.shape[0] for part in parts)
    pad = -count % 8
    if pad:
        parts = list(parts) + [jnp.zeros((pad, parts[0].shape[1]), F32)]
    return jnp.concatenate(parts, axis=0)


def plan(sizes, send_count):
    groups = LANES // send_count
    entries = []
    for block in range(27):
        off = (block // 9 - 1, block // 3 % 3 - 1, block % 3 - 1)
        if off == (0, 0, 0):
            continue
        canon = tuple(o % n for o, n in zip(off, sizes))
        for where, blocks in entries:
            if where == canon and all((b - block) % groups for b in blocks):
                blocks.append(block)
                break
        else:
            entries.append((canon, [block]))
    return entries


def kernel(
    axes, sizes, send_count,
    old_ref, move_ref, mass_ref, head_ref, tail_ref, send_ref,
    pos_ref, mult_ref,
    hot, pick, a_high, a_low, col,
    out0, in0, out1, in1, out2, in2, out3, in3, out4, in4,
    send_sem, recv_sem,
):
    atoms = old_ref.shape[-1]
    bonds = head_ref.shape[-1]
    groups = LANES // send_count
    slot_tiles = -(-27 // groups)
    slots = slot_tiles * LANES
    entries = plan(sizes, send_count)
    devices = []
    for where, _ in entries:
        if where != (0, 0, 0) and where not in devices:
            devices.append(where)
    here = [lax.axis_index(name) for name in axes]

    def target(where):
        return tuple(lax.rem(i + o, n) for i, o, n in zip(here, where, sizes))

    barrier = pltpu.get_barrier_semaphore()
    for where in devices:
        pl.semaphore_signal(barrier, inc=1, device_id=target(where), device_id_type=MESH)

    send_row = jnp.concatenate(
        [send_ref[0, 0].astype(F32), jnp.zeros((1, LANES - send_count), F32)], axis=1
    )
    send_rep = jnp.broadcast_to(send_row, (8, LANES))
    shift = send_count
    while shift < LANES:
        send_rep = send_rep + pltpu.roll(send_rep, shift, 1)
        shift *= 2
    send_col = send_rep.T[:, 0:1]
    atom_lane = lax.broadcasted_iota(jnp.int32, (1, atoms), 1).astype(F32)
    pick[...] = jnp.where(send_col == atom_lane, 1.0, 0.0).astype(BF16)

    old = jnp.concatenate([old_ref[k, 0, 0] for k in range(3)], axis=0)
    pos0 = old + jnp.concatenate([move_ref[k, 0, 0] for k in range(3)], axis=0)
    mass = mass_ref[0, 0]
    values = pieces(rows8([old, pos0, mass]))
    out0[...] = fold(dot_nt(values, pick[...]))

    if devices:
        pl.semaphore_wait(barrier, len(devices))

    def copies_same(step, source, landing):
        started = []
        for i, where in enumerate(devices):
            copy = pltpu.make_async_remote_copy(
                source, landing.at[i], send_sem.at[step, i], recv_sem.at[step, i],
                device_id=target(where), device_id_type=MESH,
            )
            copy.start()
            started.append(copy)
        return started

    def copies_each(step, source, landing):
        started = []
        for i, (where, _) in enumerate(entries):
            if where == (0, 0, 0):
                landing[i] = source[i]
                continue
            copy = pltpu.make_async_remote_copy(
                source.at[i], landing.at[i], send_sem.at[step, i], recv_sem.at[step, i],
                device_id=target(where), device_id_type=MESH,
            )
            copy.start()
            started.append(copy)
        return started

    pending = []

    def arrive(started):
        for copy in started:
            copy.wait_recv()
        pending.extend(started)

    lane_group = lax.broadcasted_iota(jnp.int32, (1, LANES), 1) // send_count

    def view(own, landing):
        tiles = []
        for q in range(slot_tiles):
            tile = jnp.zeros(own.shape, F32)
            for block in range(q * groups, min(27, (q + 1) * groups)):
                if block == 13:
                    continue
                off = (block // 9 - 1, block // 3 % 3 - 1, block % 3 - 1)
                back = tuple(-o % n for o, n in zip(off, sizes))
                data = own[...] if back == (0, 0, 0) else landing[devices.index(back)]
                tile = jnp.where(lane_group == block % groups, data, tile)
            tiles.append(tile)
        return jnp.concatenate(tiles, axis=1)

    def fill(source, rows):
        for i, (_, blocks) in enumerate(entries):
            tile = jnp.zeros((rows.shape[0], LANES), F32)
            for block in blocks:
                q = block // groups
                tile = jnp.where(
                    lane_group == block % groups, rows[:, q * LANES : (q + 1) * LANES], tile
                )
            source[i] = tile

    first = copies_same(0, out0, in0)

    head = head_ref[0, 0].astype(F32)
    tail = tail_ref[0, 0].astype(F32)
    col[...] = rows8([head, tail]).T
    wide_lane = lax.broadcasted_iota(jnp.int32, (1, atoms + slots), 1).astype(F32)
    step_rows = 16

    def hot_rows(i, carry):
        base = pl.multiple_of(i * step_rows, step_rows)
        block = col[pl.ds(base, step_rows), :]
        hot[pl.ds(base, step_rows), :] = jnp.where(block[:, 0:1] == wide_lane, 1.0, 0.0).astype(BF16)
        hot[pl.ds(bonds + base, step_rows), :] = jnp.where(
            block[:, 1:2] == wide_lane, 1.0, 0.0
        ).astype(BF16)
        return carry

    lax.fori_loop(0, bonds // step_rows, hot_rows, 0)
    ends = fold(dot_nt(values, hot[:, :atoms]))

    arrive(first)
    far = fold(dot_nt(pieces(view(out0, in0)), hot[bonds:, atoms:]))
    at_head = ends[:, :bonds]
    at_tail = ends[:, bonds:] + far
    apart = at_head - at_tail
    bond_old = apart[0:3]
    bond_new = apart[3:6]
    length = jnp.maximum(jnp.sqrt(jnp.sum(bond_old * bond_old, axis=0, keepdims=True)), 0.5)
    direction = bond_old / length
    mass_head, mass_tail = at_head[6:7], at_tail[6:7]
    scale = 1.0 / jnp.sqrt(mass_head + mass_tail)
    bent = scale * direction
    is_far = tail >= atoms
    near_mass = jnp.where(is_far, 0.0, mass_tail)
    right1 = scale * (jnp.sum(direction * bond_new, axis=0, keepdims=True) - length)

    col[...] = rows8([head, tail, mass_head, near_mass, bent]).T

    def couple_rows(i, carry):
        base = pl.multiple_of(i * step_rows, step_rows)
        block = col[pl.ds(base, step_rows), :]
        h, t, mh, mt = (block[:, k : k + 1] for k in range(4))
        same = h == head
        weight = jnp.where(same, mh, jnp.where(h == tail, -mh, 0.0)) + jnp.where(
            t == head, -mt, jnp.where(t == tail, mt, 0.0)
        )
        along = (
            block[:, 4:5] * bent[0:1] + block[:, 5:6] * bent[1:2] + block[:, 6:7] * bent[2:3]
        )
        entry = jnp.where(same, 1.0, 0.0) - along * weight
        high = entry.astype(BF16)
        a_high[pl.ds(base, step_rows), :] = high
        a_low[pl.ds(base, step_rows), :] = (entry - high.astype(F32)).astype(BF16)
        return carry

    lax.fori_loop(0, bonds // step_rows, couple_rows, 0)

    def couple(rows):
        high = rows.astype(BF16).astype(F32)
        both = jnp.concatenate([high, rows - high], axis=0).astype(BF16)
        out = dot_nn(both, a_high[...])
        count = rows.shape[0]
        return out[:count] + out[count:] + dot_nn(both, a_low[...])[:count]

    def to_slots(rows):
        return fold(dot_nn(pieces(rows), hot[bonds:, atoms:]))

    def to_bonds(rows):
        return fold(dot_nt(pieces(rows), hot[bonds:, atoms:]))

    mass_send = out0[6:7, :]

    def owner(terms, normal, response):
        moved, answers = [], []
        for k in range(ORDER + 1):
            here_k = terms[k]
            for i in range(k):
                gap = k - 1 - i
                here_k = here_k + (answers[i] if gap == 0 else response[gap - 1] * answers[i])
            total = rows8([jnp.sum(n * here_k, axis=0, keepdims=True) for n in normal])
            shift = send_count
            while shift < LANES:
                total = total + pltpu.roll(total, shift, 1)
                shift *= 2
            total = -mass_send * total
            moved.append(total[0:3])
            answers.append(sum(normal[d] * total[d : d + 1] for d in range(3)))
        return moved

    def finish(start, terms, injected):
        total = start
        for term in terms:
            total = total + term
        wave = injected[0:1]
        total = total + wave
        for k in range(1, ORDER):
            wave = couple(rows8([wave]))[0:1] + injected[k : k + 1]
            total = total + wave
        return total

    def local_series(rows):
        series = [rows]
        for _ in range(ORDER):
            series.append(couple(series[-1]))
        return series

    flags = jnp.where(is_far, 1.0, 0.0)
    series = local_series(rows8([right1, flags]))
    fixed = to_slots(rows8([bent] + [series[k][1:2] for k in range(1, ORDER)]))
    own_terms = to_slots(rows8([s[0:1] for s in series]))
    fill(out1, jnp.concatenate([fixed, own_terms], axis=0))
    second = copies_each(1, out1, in1)
    arrive(second)
    normal = [in1[:, k, :] for k in range(3)]
    response = [in1[:, 3 + k, :] for k in range(ORDER - 1)]
    moved1 = owner([in1[:, 8 + k, :] for k in range(ORDER + 1)], normal, response)
    sum1 = sum(moved1[1:], moved1[0])
    out2[...] = rows8(moved1[:ORDER] + [sum1])
    third = copies_same(2, out2, in2)
    arrive(third)

    def answer(rows):
        return [
            sum(fixed[d : d + 1] * rows[3 * k + d : 3 * k + d + 1] for d in range(3))
            for k in range(ORDER)
        ]

    seen = view(out2, in2)
    injected = to_bonds(rows8(answer(seen) + [seen[3 * ORDER : 3 * ORDER + 3]]))
    sol1 = finish(right1, [s[0:1] for s in series[1:]], injected)

    def spread(solution):
        pull = bent * solution
        both = jnp.concatenate([pull, -pull], axis=1)
        return mass * fold(dot_nn(pieces(rows8([both])), hot[:, :atoms]))[0:3]

    shift1 = spread(sol1)
    moved_ends = fold(dot_nt(pieces(rows8([shift1])), hot[:, :atoms]))[0:3]
    stretch = bond_new - (
        moved_ends[:, :bonds] - moved_ends[:, bonds:] - injected[ORDER : ORDER + 3]
    )
    current = jnp.sum(stretch * stretch, axis=0, keepdims=True)
    square = length * length
    goal = jnp.sqrt(jnp.maximum(2.0 * square - current, 0.5 * square))
    right2 = scale * (length - goal)
    series2 = local_series(rows8([right2]))
    fill(out3, to_slots(rows8([s[0:1] for s in series2])))
    fourth = copies_each(3, out3, in3)
    arrive(fourth)
    moved2 = owner([in3[:, k, :] for k in range(ORDER + 1)], normal, response)
    sum2 = sum(moved2[1:], moved2[0])
    out4[...] = rows8(moved2[:ORDER])
    fifth = copies_same(4, out4, in4)
    arrive(fifth)
    injected2 = to_bonds(rows8(answer(view(out4, in4))))
    sol2 = finish(right2, [s[0:1] for s in series2[1:]], injected2)

    once = jnp.where(lane_group == 0, sum1 + sum2, 0.0)
    at_send = fold(dot_nn(pieces(rows8([once])), pick[...]))[0:3]
    result = pos0 - shift1 - spread(sol2) - at_send
    for k in range(3):
        pos_ref[k, 0, 0] = result[k : k + 1]
    mult_ref[0, 0] = sol1 + sol2
    for copy in pending:
        copy.wait_send()


def per_device(axes, sizes, old_pos, displacement, inv_mass, bond_head, bond_tail, send_list):
    atoms, bonds, send_count = old_pos.shape[-1], bond_head.shape[-1], send_list.shape[-1]
    groups = LANES // send_count
    slots = -(-27 // groups) * LANES
    entries = plan(sizes, send_count)
    count = max(1, len(entries))
    same = max(1, len({where for where, _ in entries} - {(0, 0, 0)}))
    tile = lambda *shape: pltpu.VMEM(shape + (LANES,), F32)
    return pl.pallas_call(
        functools.partial(kernel, axes, sizes, send_count),
        out_shape=(
            jax.ShapeDtypeStruct(old_pos.shape, F32),
            jax.ShapeDtypeStruct(bond_head.shape, F32),
        ),
        in_specs=[pl.BlockSpec(memory_space=pltpu.VMEM)] * 6,
        out_specs=(pl.BlockSpec(memory_space=pltpu.VMEM), pl.BlockSpec(memory_space=pltpu.VMEM)),
        scratch_shapes=[
            pltpu.VMEM((2 * bonds, atoms + slots), BF16),
            pltpu.VMEM((LANES, atoms), BF16),
            pltpu.VMEM((bonds, bonds), BF16),
            pltpu.VMEM((bonds, bonds), BF16),
            pltpu.VMEM((bonds, 8), F32),
            tile(8), tile(same, 8),
            tile(count, 16), tile(count, 16),
            tile(16), tile(same, 16),
            tile(count, 8), tile(count, 8),
            tile(16), tile(same, 16),
            pltpu.SemaphoreType.DMA((5, count)),
            pltpu.SemaphoreType.DMA((5, count)),
        ],
        compiler_params=pltpu.CompilerParams(
            collective_id=0, has_side_effects=True, vmem_limit_bytes=56 * 1024 * 1024
        ),
    )(old_pos, displacement, inv_mass, bond_head, bond_tail, send_list)


def solution(mesh):
    axes = ("gx", "gy", "gz")
    sizes = tuple(mesh.shape[name] for name in axes)
    return jax.shard_map(
        functools.partial(per_device, axes, sizes),
        mesh=mesh,
        in_specs=(
            P(None, "gx", "gy", "gz", None),
            P(None, "gx", "gy", "gz", None),
            P("gx", "gy", "gz", None),
            P("gx", "gy", "gz", None),
            P("gx", "gy", "gz", None),
            P("gx", "gy", "gz", None),
        ),
        out_specs=(P(None, "gx", "gy", "gz", None), P("gx", "gy", "gz", None)),
        check_vma=False,
    )
```

```python
import functools
import itertools

import jax
import jax.numpy as jnp
from jax import lax
from jax.experimental import pallas as pl
from jax.experimental.pallas import tpu as pltpu
from jax.sharding import PartitionSpec as P

ORDER = 4
LANES = 128
F32, BF16 = jnp.float32, jnp.bfloat16
MESH = pl.DeviceIdType.MESH


def pieces(value):
    high = value.astype(BF16).astype(F32)
    rest = value - high
    middle = rest.astype(BF16).astype(F32)
    return jnp.concatenate([high, middle, rest - middle], axis=0).astype(BF16)


def fold(out):
    rows = out.shape[0] // 3
    return out[:rows] + out[rows : 2 * rows] + out[2 * rows :]


def dot_nt(left, right):
    return lax.dot_general(left, right, (((1,), (1,)), ((), ())), preferred_element_type=F32)


def dot_nn(left, right):
    return lax.dot_general(left, right, (((1,), (0,)), ((), ())), preferred_element_type=F32)


def rows8(parts):
    count = sum(part.shape[0] for part in parts)
    pad = -count % 8
    if pad:
        parts = list(parts) + [jnp.zeros((pad, parts[0].shape[1]), F32)]
    return jnp.concatenate(parts, axis=0)


def plan(sizes, send_count):
    groups = LANES // send_count
    entries = []
    for block in range(27):
        off = (block // 9 - 1, block // 3 % 3 - 1, block % 3 - 1)
        if off == (0, 0, 0):
            continue
        canon = tuple(o % n for o, n in zip(off, sizes))
        for where, blocks in entries:
            if where == canon and all((b - block) % groups for b in blocks):
                blocks.append(block)
                break
        else:
            entries.append((canon, [block]))
    return entries


def kernel(
    axes, sizes, send_count,
    old_ref, move_ref, mass_ref, head_ref, tail_ref, send_ref,
    pos_ref, mult_ref,
    hot_head, ends, pick, above, beside, root, col,
    out0, in0, out1, in1, out2, in2, out3, in3, out4, in4,
    send_sem, recv_sem,
):
    atoms = old_ref.shape[-1]
    bonds = head_ref.shape[-1]
    groups = LANES // send_count
    slot_tiles = -(-27 // groups)
    slots = slot_tiles * LANES
    entries = plan(sizes, send_count)
    devices = []
    for where, _ in entries:
        if where != (0, 0, 0) and where not in devices:
            devices.append(where)
    here = [lax.axis_index(name) for name in axes]

    def target(where):
        return tuple(lax.rem(i + o, n) for i, o, n in zip(here, where, sizes))

    barrier = pltpu.get_barrier_semaphore()
    for where in devices:
        pl.semaphore_signal(barrier, inc=1, device_id=target(where), device_id_type=MESH)

    send_row = jnp.concatenate(
        [send_ref[0, 0].astype(F32), jnp.zeros((1, LANES - send_count), F32)], axis=1
    )
    send_rep = jnp.broadcast_to(send_row, (8, LANES))
    shift = send_count
    while shift < LANES:
        send_rep = send_rep + pltpu.roll(send_rep, shift, 1)
        shift *= 2
    send_col = send_rep.T[:, 0:1]
    atom_lane = lax.broadcasted_iota(jnp.int32, (1, atoms), 1).astype(F32)
    pick[...] = jnp.where(send_col == atom_lane, 1.0, 0.0).astype(BF16)

    old = jnp.concatenate([old_ref[k, 0, 0] for k in range(3)], axis=0)
    pos0 = old + jnp.concatenate([move_ref[k, 0, 0] for k in range(3)], axis=0)
    mass = mass_ref[0, 0]
    values = pieces(rows8([old, pos0, mass]))
    out0[...] = fold(dot_nt(values, pick[...]))

    if devices:
        pl.semaphore_wait(barrier, len(devices))

    def copies_same(step, source, landing):
        started = []
        for i, where in enumerate(devices):
            copy = pltpu.make_async_remote_copy(
                source, landing.at[i], send_sem.at[step, i], recv_sem.at[step, i],
                device_id=target(where), device_id_type=MESH,
            )
            copy.start()
            started.append(copy)
        return started

    def copies_each(step, source, landing):
        started = []
        for i, (where, _) in enumerate(entries):
            if where == (0, 0, 0):
                landing[i] = source[i]
                continue
            copy = pltpu.make_async_remote_copy(
                source.at[i], landing.at[i], send_sem.at[step, i], recv_sem.at[step, i],
                device_id=target(where), device_id_type=MESH,
            )
            copy.start()
            started.append(copy)
        return started

    pending = []

    def arrive(started):
        for copy in started:
            copy.wait_recv()
        pending.extend(started)

    lane_group = lax.broadcasted_iota(jnp.int32, (1, LANES), 1) // send_count

    def view(own, landing):
        tiles = []
        for q in range(slot_tiles):
            tile = jnp.zeros(own.shape, F32)
            for block in range(q * groups, min(27, (q + 1) * groups)):
                if block == 13:
                    continue
                off = (block // 9 - 1, block // 3 % 3 - 1, block % 3 - 1)
                back = tuple(-o % n for o, n in zip(off, sizes))
                data = own[...] if back == (0, 0, 0) else landing[devices.index(back)]
                tile = jnp.where(lane_group == block % groups, data, tile)
            tiles.append(tile)
        return jnp.concatenate(tiles, axis=1)

    def fill(source, rows):
        for i, (_, blocks) in enumerate(entries):
            tile = jnp.zeros((rows.shape[0], LANES), F32)
            for block in blocks:
                q = block // groups
                tile = jnp.where(
                    lane_group == block % groups, rows[:, q * LANES : (q + 1) * LANES], tile
                )
            source[i] = tile

    first = copies_same(0, out0, in0)

    head = head_ref[0, 0].astype(F32)
    tail = tail_ref[0, 0].astype(F32)
    col[...] = rows8([head, tail]).T
    wide_lane = lax.broadcasted_iota(jnp.int32, (1, atoms + slots), 1).astype(F32)
    step_rows = 16

    def index_rows(i, carry):
        base = pl.multiple_of(i * step_rows, step_rows)
        block = col[pl.ds(base, step_rows), :]
        h, t = block[:, 0:1], block[:, 1:2]
        at_h = h == atom_lane
        hot_head[pl.ds(base, step_rows), :] = jnp.where(at_h, 1.0, 0.0).astype(BF16)
        ends[pl.ds(base, step_rows), :] = jnp.where(
            h == wide_lane, 1.0, jnp.where(t == wide_lane, -1.0, 0.0)
        ).astype(BF16)
        above[pl.ds(base, step_rows), :] = jnp.where(t == head, 1.0, 0.0).astype(BF16)
        beside[pl.ds(base, step_rows), :] = jnp.where(
            t == tail, 1.0, jnp.where(h == tail, -1.0, 0.0)
        ).astype(BF16)
        return carry

    lax.fori_loop(0, bonds // step_rows, index_rows, 0)
    apart = fold(dot_nt(values, ends[:, :atoms]))
    mass_head = fold(dot_nt(pieces(rows8([mass])), hot_head[...]))[0:1]
    is_far = tail >= atoms
    flags = jnp.where(is_far, 1.0, 0.0)

    def climb(label):
        rows = jnp.broadcast_to(label, (8, bonds))
        high = rows.astype(BF16).astype(F32)
        both = jnp.concatenate([high, rows - high], axis=0).astype(BF16)
        out = dot_nt(both, above[...])
        return jnp.where(is_far, tail, out[0:1] + out[8:9])

    def mark(label):
        col[:, 0:8] = jnp.broadcast_to(label, (8, bonds)).T
        slot_lane = (lax.broadcasted_iota(jnp.int32, (1, slots), 1) + atoms).astype(F32)

        def mark_rows(i, carry):
            base = pl.multiple_of(i * 32, 32)
            block = col[pl.ds(base, 32), :]
            root[pl.ds(base, 32), :] = jnp.where(block[:, 0:1] == slot_lane, 1.0, 0.0).astype(BF16)
            return carry

        lax.fori_loop(0, bonds // 32, mark_rows, 0)

    label = jnp.where(is_far, tail, 0.0)
    for _ in range(ORDER // 2):
        label = climb(label)
    mark(label)

    arrive(first)
    apart = apart + fold(dot_nt(pieces(view(out0, in0)), ends[:, atoms:]))
    bond_old = apart[0:3]
    bond_new = apart[3:6]
    length = jnp.maximum(jnp.sqrt(jnp.sum(bond_old * bond_old, axis=0, keepdims=True)), 0.5)
    direction = bond_old / length
    mass_tail = mass_head - apart[6:7]
    scale = 1.0 / jnp.sqrt(mass_head + mass_tail)
    bent = scale * direction
    near_mass = jnp.where(is_far, 0.0, mass_tail)
    right1 = scale * (jnp.sum(direction * bond_new, axis=0, keepdims=True) - length)

    def meet(pull):
        rows = rows8([pull])
        count = rows.shape[0]
        high = rows.astype(BF16).astype(F32)
        both = jnp.concatenate([high, rows - high], axis=0).astype(BF16)
        up = dot_nn(both, above[...])
        side = dot_nn(both, beside[...])
        out = mass_head * (rows - up[:count] - up[count:]) + near_mass * (side[:count] + side[count:])
        return out[: pull.shape[0]]

    def couple(*rows):
        out = meet(jnp.concatenate([bent * row for row in rows], axis=0))
        return [
            row - jnp.sum(bent * out[3 * k : 3 * k + 3], axis=0, keepdims=True)
            for k, row in enumerate(rows)
        ]

    def to_slots(rows):
        return fold(dot_nn(pieces(rows8(rows)), root[...]))

    def to_bonds(rows):
        return fold(dot_nt(pieces(rows8(rows)), root[...]))

    mass_send = out0[6:7, :]

    def owner(terms, normal, response):
        moved, answers = [], []
        for k in range(ORDER + 1):
            here_k = terms[k]
            for i in range(k):
                gap = k - 1 - i
                here_k = here_k + (answers[i] if gap == 0 else response[gap - 1] * answers[i])
            total = rows8([jnp.sum(n * here_k, axis=0, keepdims=True) for n in normal])
            shift = send_count
            while shift < LANES:
                total = total + pltpu.roll(total, shift, 1)
                shift *= 2
            total = -mass_send * total
            moved.append(total[0:3])
            answers.append(sum(normal[d] * total[d : d + 1] for d in range(3)))
        return moved

    def through(injected):
        total = 0.0
        weight = 0.0
        for k in range(ORDER):
            weight = weight + far_terms[k]
            total = total + weight * injected[ORDER - 1 - k : ORDER - k]
        return total

    terms1, far_terms = [right1], [flags]
    half = ORDER // 2
    for _ in range(half):
        near, far = couple(terms1[-1], far_terms[-1])
        terms1.append(near)
        far_terms.append(far)

    def at_far(terms, k):
        return far_terms[max(0, k - half)] * terms[min(k, half)]

    fixed = to_slots([bent * flags] + [at_far(far_terms, k) for k in range(1, ORDER)])
    own_terms = to_slots([at_far(terms1, k) for k in range(ORDER + 1)])
    fill(out1, jnp.concatenate([fixed, own_terms], axis=0))
    second = copies_each(1, out1, in1)
    for _ in range(ORDER - half):
        near, far = couple(terms1[-1], far_terms[-1])
        terms1.append(near)
        far_terms.append(far)
        label = climb(label)
    mark(label)
    base1 = sum(terms1[1:], terms1[0])
    arrive(second)
    normal = [in1[:, k, :] for k in range(3)]
    response = [in1[:, 3 + k, :] for k in range(ORDER - 1)]
    moved1 = owner([in1[:, 8 + k, :] for k in range(ORDER + 1)], normal, response)
    sum1 = sum(moved1[1:], moved1[0])
    out2[...] = rows8(moved1[:ORDER] + [sum1])
    third = copies_same(2, out2, in2)
    arrive(third)

    def answer(rows):
        return [
            sum(fixed[d : d + 1] * rows[3 * k + d : 3 * k + d + 1] for d in range(3))
            for k in range(ORDER)
        ]

    seen = view(out2, in2)
    injected = to_bonds(answer(seen) + [seen[3 * ORDER : 3 * ORDER + 3]])
    sol1 = base1 + through(injected)
    stretch = bond_new - (meet(bent * sol1) - flags * injected[ORDER : ORDER + 3])
    current = jnp.sum(stretch * stretch, axis=0, keepdims=True)
    square = length * length
    goal = jnp.sqrt(jnp.maximum(2.0 * square - current, 0.5 * square))
    right2 = scale * (length - goal)
    fill(out3, to_slots([far_terms[k] * right2 for k in range(ORDER + 1)]))
    fourth = copies_each(3, out3, in3)
    term, both = right2, sol1 + right2
    for _ in range(half):
        (term,) = couple(term)
        both = both + term
    arrive(fourth)
    moved2 = owner([in3[:, k, :] for k in range(ORDER + 1)], normal, response)
    sum2 = sum(moved2[1:], moved2[0])
    out4[...] = rows8(moved2[:ORDER])
    fifth = copies_same(4, out4, in4)
    for _ in range(ORDER - half):
        (term,) = couple(term)
        both = both + term
    once = jnp.where(lane_group == 0, sum1 + sum2, 0.0)
    start = pos0 - fold(dot_nn(pieces(rows8([once])), pick[...]))[0:3]
    arrive(fifth)
    both = both + through(to_bonds(answer(view(out4, in4))))
    mult_ref[0, 0] = both
    result = start - mass * fold(dot_nn(pieces(rows8([bent * both])), ends[:, :atoms]))[0:3]
    for k in range(3):
        pos_ref[k, 0, 0] = result[k : k + 1]
    for copy in pending:
        copy.wait_send()


def per_device(axes, sizes, old_pos, displacement, inv_mass, bond_head, bond_tail, send_list):
    atoms, bonds, send_count = old_pos.shape[-1], bond_head.shape[-1], send_list.shape[-1]
    groups = LANES // send_count
    slots = -(-27 // groups) * LANES
    entries = plan(sizes, send_count)
    count = max(1, len(entries))
    same = max(1, len({where for where, _ in entries} - {(0, 0, 0)}))
    tile = lambda *shape: pltpu.VMEM(shape + (LANES,), F32)
    return pl.pallas_call(
        functools.partial(kernel, axes, sizes, send_count),
        out_shape=(
            jax.ShapeDtypeStruct(old_pos.shape, F32),
            jax.ShapeDtypeStruct(bond_head.shape, F32),
        ),
        in_specs=[pl.BlockSpec(memory_space=pltpu.VMEM)] * 6,
        out_specs=(pl.BlockSpec(memory_space=pltpu.VMEM), pl.BlockSpec(memory_space=pltpu.VMEM)),
        scratch_shapes=[
            pltpu.VMEM((bonds, atoms), BF16),
            pltpu.VMEM((bonds, atoms + slots), BF16),
            pltpu.VMEM((LANES, atoms), BF16),
            pltpu.VMEM((bonds, bonds), BF16),
            pltpu.VMEM((bonds, bonds), BF16),
            pltpu.VMEM((bonds, slots), BF16),
            pltpu.VMEM((bonds, 8), F32),
            tile(8), tile(same, 8),
            tile(count, 16), tile(count, 16),
            tile(16), tile(same, 16),
            tile(count, 8), tile(count, 8),
            tile(16), tile(same, 16),
            pltpu.SemaphoreType.DMA((5, count)),
            pltpu.SemaphoreType.DMA((5, count)),
        ],
        compiler_params=pltpu.CompilerParams(
            collective_id=0, has_side_effects=True, vmem_limit_bytes=56 * 1024 * 1024
        ),
    )(old_pos, displacement, inv_mass, bond_head, bond_tail, send_list)


def solution(mesh):
    axes = ("gx", "gy", "gz")
    sizes = tuple(mesh.shape[name] for name in axes)
    return jax.shard_map(
        functools.partial(per_device, axes, sizes),
        mesh=mesh,
        in_specs=(
            P(None, "gx", "gy", "gz", None),
            P(None, "gx", "gy", "gz", None),
            P("gx", "gy", "gz", None),
            P("gx", "gy", "gz", None),
            P("gx", "gy", "gz", None),
            P("gx", "gy", "gz", None),
        ),
        out_specs=(P(None, "gx", "gy", "gz", None), P("gx", "gy", "gz", None)),
        check_vma=False,
    )
```

```python
import functools
import itertools

import jax
import jax.numpy as jnp
from jax import lax
from jax.experimental import pallas as pl
from jax.experimental.pallas import tpu as pltpu
from jax.sharding import PartitionSpec as P

ORDER = 4
LANES = 128
F32, BF16 = jnp.float32, jnp.bfloat16
MESH = pl.DeviceIdType.MESH


def pieces(value):
    high = value.astype(BF16).astype(F32)
    rest = value - high
    middle = rest.astype(BF16).astype(F32)
    return jnp.concatenate([high, middle, rest - middle], axis=0).astype(BF16)


def fold(out):
    rows = out.shape[0] // 3
    return out[:rows] + out[rows : 2 * rows] + out[2 * rows :]


def dot_nt(left, right):
    return lax.dot_general(left, right, (((1,), (1,)), ((), ())), preferred_element_type=F32)


def dot_nn(left, right):
    return lax.dot_general(left, right, (((1,), (0,)), ((), ())), preferred_element_type=F32)


def rows8(parts):
    count = sum(part.shape[0] for part in parts)
    pad = -count % 8
    if pad:
        parts = list(parts) + [jnp.zeros((pad, parts[0].shape[1]), F32)]
    return jnp.concatenate(parts, axis=0)


def plan(sizes, send_count):
    groups = LANES // send_count
    entries = []
    for block in range(27):
        off = (block // 9 - 1, block // 3 % 3 - 1, block % 3 - 1)
        if off == (0, 0, 0):
            continue
        canon = tuple(o % n for o, n in zip(off, sizes))
        for where, blocks in entries:
            if where == canon and all((b - block) % groups for b in blocks):
                blocks.append(block)
                break
        else:
            entries.append((canon, [block]))
    return entries


def kernel(
    axes, sizes, send_count,
    old_ref, move_ref, mass_ref, head_ref, tail_ref, send_ref,
    pos_ref, mult_ref,
    low, pick, above, beside, root, col,
    out0, in0, out1, in1, out2, in2, out3, in3, out4, in4,
    send_sem, recv_sem,
):
    atoms = old_ref.shape[-1]
    bonds = head_ref.shape[-1]
    groups = LANES // send_count
    slot_tiles = -(-27 // groups)
    slots = slot_tiles * LANES
    entries = plan(sizes, send_count)
    devices = []
    for where, _ in entries:
        if where != (0, 0, 0) and where not in devices:
            devices.append(where)
    here = [lax.axis_index(name) for name in axes]

    def target(where):
        return tuple(lax.rem(i + o, n) for i, o, n in zip(here, where, sizes))

    barrier = pltpu.get_barrier_semaphore()
    for where in devices:
        pl.semaphore_signal(barrier, inc=1, device_id=target(where), device_id_type=MESH)

    send_row = jnp.concatenate(
        [send_ref[0, 0].astype(F32), jnp.zeros((1, LANES - send_count), F32)], axis=1
    )
    send_rep = jnp.broadcast_to(send_row, (8, LANES))
    shift = send_count
    while shift < LANES:
        send_rep = send_rep + pltpu.roll(send_rep, shift, 1)
        shift *= 2
    send_col = send_rep.T[:, 0:1]
    atom_lane = lax.broadcasted_iota(jnp.int32, (1, atoms), 1).astype(F32)
    pick[...] = jnp.where(send_col == atom_lane, 1.0, 0.0).astype(BF16)

    old = jnp.concatenate([old_ref[k, 0, 0] for k in range(3)], axis=0)
    pos0 = old + jnp.concatenate([move_ref[k, 0, 0] for k in range(3)], axis=0)
    mass = mass_ref[0, 0]
    data = rows8([old, pos0, mass])
    out0[...] = fold(dot_nt(pieces(data), pick[...]))

    if devices:
        pl.semaphore_wait(barrier, len(devices))

    def copies_same(step, source, landing):
        started = []
        for i, where in enumerate(devices):
            copy = pltpu.make_async_remote_copy(
                source, landing.at[i], send_sem.at[step, i], recv_sem.at[step, i],
                device_id=target(where), device_id_type=MESH,
            )
            copy.start()
            started.append(copy)
        return started

    def copies_each(step, source, landing):
        started = []
        for i, (where, _) in enumerate(entries):
            if where == (0, 0, 0):
                landing[i] = source[i]
                continue
            copy = pltpu.make_async_remote_copy(
                source.at[i], landing.at[i], send_sem.at[step, i], recv_sem.at[step, i],
                device_id=target(where), device_id_type=MESH,
            )
            copy.start()
            started.append(copy)
        return started

    pending = []

    def arrive(started):
        for copy in started:
            copy.wait_recv()
        pending.extend(started)

    lane_group = lax.broadcasted_iota(jnp.int32, (1, LANES), 1) // send_count

    def view(own, landing):
        tiles = []
        for q in range(slot_tiles):
            tile = jnp.zeros(own.shape, F32)
            for block in range(q * groups, min(27, (q + 1) * groups)):
                if block == 13:
                    continue
                off = (block // 9 - 1, block // 3 % 3 - 1, block % 3 - 1)
                back = tuple(-o % n for o, n in zip(off, sizes))
                data = own[...] if back == (0, 0, 0) else landing[devices.index(back)]
                tile = jnp.where(lane_group == block % groups, data, tile)
            tiles.append(tile)
        return jnp.concatenate(tiles, axis=1)

    def fill(source, rows):
        for i, (_, blocks) in enumerate(entries):
            tile = jnp.zeros((rows.shape[0], LANES), F32)
            for block in blocks:
                q = block // groups
                tile = jnp.where(
                    lane_group == block % groups, rows[:, q * LANES : (q + 1) * LANES], tile
                )
            source[i] = tile

    first = copies_same(0, out0, in0)

    head = head_ref[0, 0].astype(F32)
    tail = tail_ref[0, 0].astype(F32)
    end_atom = jnp.concatenate([head_ref[0, 0], tail_ref[0, 0]], axis=1)
    end_tile = (end_atom // LANES).astype(F32)
    end_lane = (end_atom % LANES).astype(F32)
    col[...] = rows8([head, tail, end_lane[:, :bonds], end_lane[:, bonds:]]).T
    one_lane = lax.broadcasted_iota(jnp.int32, (1, LANES), 1).astype(F32)
    atom_tiles = atoms // LANES
    step_rows = 16

    def index_rows(i, carry):
        base = pl.multiple_of(i * step_rows, step_rows)
        block = col[pl.ds(base, step_rows), :]
        h, t = block[:, 0:1], block[:, 1:2]
        low[pl.ds(base, step_rows), :] = jnp.where(block[:, 2:3] == one_lane, 1.0, 0.0).astype(BF16)
        low[pl.ds(bonds + base, step_rows), :] = jnp.where(
            block[:, 3:4] == one_lane, 1.0, 0.0
        ).astype(BF16)
        above[pl.ds(base, step_rows), :] = jnp.where(t == head, 1.0, 0.0).astype(BF16)
        beside[pl.ds(base, step_rows), :] = jnp.where(
            t == tail, 1.0, jnp.where(h == tail, -1.0, 0.0)
        ).astype(BF16)
        return carry

    lax.fori_loop(0, bonds // step_rows, index_rows, 0)

    def take(rows, hot, where, base):
        tiles = rows.shape[1] // LANES
        stacked = jnp.concatenate(
            [rows[:, k * LANES : (k + 1) * LANES] for k in range(tiles)], axis=0
        )
        found = fold(dot_nt(pieces(stacked), hot))
        total = jnp.zeros((8, hot.shape[0]), F32)
        for k in range(tiles):
            total = jnp.where(where == base + k, found[8 * k : 8 * k + 8], total)
        return total

    at_ends = take(data, low[...], end_tile, 0)
    is_far = tail >= atoms
    flags = jnp.where(is_far, 1.0, 0.0)

    def climb(label):
        rows = jnp.broadcast_to(label, (8, bonds))
        high = rows.astype(BF16).astype(F32)
        both = jnp.concatenate([high, rows - high], axis=0).astype(BF16)
        out = dot_nt(both, above[...])
        return jnp.where(is_far, tail, out[0:1] + out[8:9])

    def mark(label):
        col[:, 0:8] = jnp.broadcast_to(label, (8, bonds)).T
        slot_lane = (lax.broadcasted_iota(jnp.int32, (1, slots), 1) + atoms).astype(F32)

        def mark_rows(i, carry):
            base = pl.multiple_of(i * 32, 32)
            block = col[pl.ds(base, 32), :]
            root[pl.ds(base, 32), :] = jnp.where(block[:, 0:1] == slot_lane, 1.0, 0.0).astype(BF16)
            return carry

        lax.fori_loop(0, bonds // 32, mark_rows, 0)

    label = jnp.where(is_far, tail, 0.0)
    for _ in range(ORDER // 2):
        label = climb(label)
    mark(label)

    arrive(first)
    at_tail = at_ends[:, bonds:] + take(
        view(out0, in0), low[bonds:, :], end_tile[:, bonds:], atom_tiles
    )
    apart = at_ends[:, :bonds] - at_tail
    mass_head, mass_tail = at_ends[6:7, :bonds], at_tail[6:7]
    bond_old = apart[0:3]
    bond_new = apart[3:6]
    length = jnp.maximum(jnp.sqrt(jnp.sum(bond_old * bond_old, axis=0, keepdims=True)), 0.5)
    direction = bond_old / length
    scale = 1.0 / jnp.sqrt(mass_head + mass_tail)
    bent = scale * direction
    near_mass = jnp.where(is_far, 0.0, mass_tail)
    right1 = scale * (jnp.sum(direction * bond_new, axis=0, keepdims=True) - length)

    def meet(pull):
        rows = rows8([pull])
        count = rows.shape[0]
        high = rows.astype(BF16).astype(F32)
        both = jnp.concatenate([high, rows - high], axis=0).astype(BF16)
        up = dot_nn(both, above[...])
        side = dot_nn(both, beside[...])
        out = mass_head * (rows - up[:count] - up[count:]) + near_mass * (side[:count] + side[count:])
        return out[: pull.shape[0]]

    def couple(*rows):
        out = meet(jnp.concatenate([bent * row for row in rows], axis=0))
        return [
            row - jnp.sum(bent * out[3 * k : 3 * k + 3], axis=0, keepdims=True)
            for k, row in enumerate(rows)
        ]

    def to_slots(rows):
        return fold(dot_nn(pieces(rows8(rows)), root[...]))

    def to_bonds(rows):
        return fold(dot_nt(pieces(rows8(rows)), root[...]))

    mass_send = out0[6:7, :]

    def owner(terms, normal, response):
        moved, answers = [], []
        for k in range(ORDER + 1):
            here_k = terms[k]
            for i in range(k):
                gap = k - 1 - i
                here_k = here_k + (answers[i] if gap == 0 else response[gap - 1] * answers[i])
            total = rows8([jnp.sum(n * here_k, axis=0, keepdims=True) for n in normal])
            shift = send_count
            while shift < LANES:
                total = total + pltpu.roll(total, shift, 1)
                shift *= 2
            total = -mass_send * total
            moved.append(total[0:3])
            answers.append(sum(normal[d] * total[d : d + 1] for d in range(3)))
        return moved

    def through(injected):
        total = 0.0
        weight = 0.0
        for k in range(ORDER):
            weight = weight + far_terms[k]
            total = total + weight * injected[ORDER - 1 - k : ORDER - k]
        return total

    terms1, far_terms = [right1], [flags]
    half = ORDER // 2
    for _ in range(half):
        near, far = couple(terms1[-1], far_terms[-1])
        terms1.append(near)
        far_terms.append(far)

    def at_far(terms, k):
        return far_terms[max(0, k - half)] * terms[min(k, half)]

    fixed = to_slots([bent * flags] + [at_far(far_terms, k) for k in range(1, ORDER)])
    own_terms = to_slots([at_far(terms1, k) for k in range(ORDER + 1)])
    fill(out1, jnp.concatenate([fixed, own_terms], axis=0))
    second = copies_each(1, out1, in1)

    def longer(steps, label):
        for _ in range(steps):
            near, far = couple(terms1[-1], far_terms[-1])
            terms1.append(near)
            far_terms.append(far)
            label = climb(label)
        return label

    label = longer((ORDER - half) // 2, label)
    arrive(second)
    normal = [in1[:, k, :] for k in range(3)]
    response = [in1[:, 3 + k, :] for k in range(ORDER - 1)]
    moved1 = owner([in1[:, 8 + k, :] for k in range(ORDER + 1)], normal, response)
    sum1 = sum(moved1[1:], moved1[0])
    out2[...] = rows8(moved1[:ORDER] + [sum1])
    third = copies_same(2, out2, in2)
    mark(longer(ORDER - half - (ORDER - half) // 2, label))
    base1 = sum(terms1[1:], terms1[0])
    arrive(third)

    def answer(rows):
        return [
            sum(fixed[d : d + 1] * rows[3 * k + d : 3 * k + d + 1] for d in range(3))
            for k in range(ORDER)
        ]

    seen = view(out2, in2)
    injected = to_bonds(answer(seen) + [seen[3 * ORDER : 3 * ORDER + 3]])
    sol1 = base1 + through(injected)
    stretch = bond_new - (meet(bent * sol1) - flags * injected[ORDER : ORDER + 3])
    current = jnp.sum(stretch * stretch, axis=0, keepdims=True)
    square = length * length
    goal = jnp.sqrt(jnp.maximum(2.0 * square - current, 0.5 * square))
    right2 = scale * (length - goal)
    fill(out3, to_slots([far_terms[k] * right2 for k in range(ORDER + 1)]))
    fourth = copies_each(3, out3, in3)
    term, both = right2, sol1 + right2
    for _ in range(half):
        (term,) = couple(term)
        both = both + term
    arrive(fourth)
    moved2 = owner([in3[:, k, :] for k in range(ORDER + 1)], normal, response)
    sum2 = sum(moved2[1:], moved2[0])
    out4[...] = rows8(moved2[:ORDER])
    fifth = copies_same(4, out4, in4)
    for _ in range(ORDER - half):
        (term,) = couple(term)
        both = both + term
    once = jnp.where(lane_group == 0, sum1 + sum2, 0.0)
    start = pos0 - fold(dot_nn(pieces(rows8([once])), pick[...]))[0:3]
    arrive(fifth)
    both = both + through(to_bonds(answer(view(out4, in4))))
    mult_ref[0, 0] = both
    pull = bent * both
    parts = pieces(rows8([jnp.concatenate([pull, -pull], axis=1)])).astype(F32)
    kept = jnp.concatenate(
        [jnp.where(end_tile == k, parts, 0.0) for k in range(atom_tiles)], axis=0
    )
    added = dot_nn(kept.astype(BF16), low[...])
    added = jnp.concatenate(
        [fold(added[24 * k : 24 * k + 24]) for k in range(atom_tiles)], axis=1
    )
    result = start - mass * added[0:3]
    for k in range(3):
        pos_ref[k, 0, 0] = result[k : k + 1]
    for copy in pending:
        copy.wait_send()


def per_device(axes, sizes, old_pos, displacement, inv_mass, bond_head, bond_tail, send_list):
    atoms, bonds, send_count = old_pos.shape[-1], bond_head.shape[-1], send_list.shape[-1]
    groups = LANES // send_count
    slots = -(-27 // groups) * LANES
    entries = plan(sizes, send_count)
    count = max(1, len(entries))
    same = max(1, len({where for where, _ in entries} - {(0, 0, 0)}))
    tile = lambda *shape: pltpu.VMEM(shape + (LANES,), F32)
    return pl.pallas_call(
        functools.partial(kernel, axes, sizes, send_count),
        out_shape=(
            jax.ShapeDtypeStruct(old_pos.shape, F32),
            jax.ShapeDtypeStruct(bond_head.shape, F32),
        ),
        in_specs=[pl.BlockSpec(memory_space=pltpu.VMEM)] * 6,
        out_specs=(pl.BlockSpec(memory_space=pltpu.VMEM), pl.BlockSpec(memory_space=pltpu.VMEM)),
        scratch_shapes=[
            pltpu.VMEM((2 * bonds, LANES), BF16),
            pltpu.VMEM((LANES, atoms), BF16),
            pltpu.VMEM((bonds, bonds), BF16),
            pltpu.VMEM((bonds, bonds), BF16),
            pltpu.VMEM((bonds, slots), BF16),
            pltpu.VMEM((bonds, 8), F32),
            tile(8), tile(same, 8),
            tile(count, 16), tile(count, 16),
            tile(16), tile(same, 16),
            tile(count, 8), tile(count, 8),
            tile(16), tile(same, 16),
            pltpu.SemaphoreType.DMA((5, count)),
            pltpu.SemaphoreType.DMA((5, count)),
        ],
        compiler_params=pltpu.CompilerParams(
            collective_id=0, has_side_effects=True, vmem_limit_bytes=56 * 1024 * 1024
        ),
    )(old_pos, displacement, inv_mass, bond_head, bond_tail, send_list)


def solution(mesh):
    axes = ("gx", "gy", "gz")
    sizes = tuple(mesh.shape[name] for name in axes)
    return jax.shard_map(
        functools.partial(per_device, axes, sizes),
        mesh=mesh,
        in_specs=(
            P(None, "gx", "gy", "gz", None),
            P(None, "gx", "gy", "gz", None),
            P("gx", "gy", "gz", None),
            P("gx", "gy", "gz", None),
            P("gx", "gy", "gz", None),
            P("gx", "gy", "gz", None),
        ),
        out_specs=(P(None, "gx", "gy", "gz", None), P("gx", "gy", "gz", None)),
        check_vma=False,
    )
```
